32 devices in a mesh: seq: 8 (over z, y), grp: 4 (over x, core).
Axes of the slice: x: 2, y: 2, z: 4, core: 2. Of those that a mesh axis runs over, the one named last changes fastest.
Arguments:
- frames: bfloat16 [16384, 1024], P(('seq', 'grp')), may hold values from -6 to 6
- ln1_gain: float32 [1024], replicated, may hold values from 0.1 to 1.9
- w_in: bfloat16 [1024, 2, 1024], P('seq', None, 'grp'), may hold values from -0.1875 to 0.1875
- w_dw: bfloat16 [31, 1024], replicated, may hold values from -1 to 1
- ln2_gain: float32 [1024], replicated, may hold values from 0.1 to 1.9
- ln2_bias: float32 [1024], replicated, may hold values from -3 to 3
- w_out: bfloat16 [1024, 1024], P('grp', 'seq'), may hold values from -0.1875 to 0.1875
- block_utt: int32 [128], replicated, may hold values from 0 to 31, as said below
- block_off: int32 [128], replicated, may hold values from 0 to 6, as said below
- lengths: int32 [32], replicated, may hold values from 1 to 896, as said below
Outputs:
- result: bfloat16 [16384, 1024], P(('seq', 'grp'))
The draws below stay inside these ranges and needn't reach their ends.
Inputs may be any that keep to these rules, and one draw needn't show every extreme that they name: block_utt never falls along the blocks and names every utterance; each utterance is one run of 1 to 7 whole blocks, and some utterance has exactly 7. block_off counts the blocks of the run before a block, starting at 0. `lengths`: an utterance of n blocks has more than (n - 1) * 128 and at most n * 128 live frames.
All inputs are finite; a program needn't handle non-finite values.
Results may differ from the reference program's by a relative error of at most 0.0046.
Values may be sent and summed in bfloat16 or wider, within the bound.
A program may use at most 64 MiB of HBM per device.

```python
import jax
import jax.numpy as jnp
from jax import lax

D = 1024
KER = 31
BLK = 128
FRAMES = 16384
NBLK = 128
UTTS = 32
N_SEQ = 8


def layout_tables(key):
    base = jax.random.fold_in(key, 7)
    first_key, second_key = jax.random.split(base)
    pattern = jnp.array([-3, -2, -1, 0, 0, 1, 2, 3], jnp.int32)
    offsets = jnp.tile(pattern, UTTS // 8)
    order = jax.random.permutation(first_key, UTTS)
    counts = (4 + jnp.take(offsets, order)).astype(jnp.int32)
    ends = jnp.cumsum(counts).astype(jnp.int32)
    starts = (ends - counts).astype(jnp.int32)
    indices = jnp.arange(NBLK, dtype=jnp.int32)
    block_utt = jnp.sum((ends[None, :] <= indices[:, None]).astype(jnp.int32), axis=1).astype(jnp.int32)
    block_off = (indices - jnp.take(starts, block_utt)).astype(jnp.int32)
    tails = jax.random.randint(second_key, (UTTS,), 1, BLK + 1, dtype=jnp.int32)
    tails = jnp.where(counts == 7, BLK, tails).astype(jnp.int32)
    lengths = ((counts - 1) * BLK + tails).astype(jnp.int32)
    return (block_utt, block_off, lengths)


def draw_block_utt(key, part):
    return layout_tables(key)[0]


def draw_block_off(key, part):
    return layout_tables(key)[1]


def draw_lengths(key, part):
    return layout_tables(key)[2]


def shard_levels(rng, shape, shards, least, high):
    level = 1.0
    for dim, shards_of in shards:
        steps = jax.random.uniform(jax.random.fold_in(jax.random.fold_in(rng, 6), dim), (shards_of,), jnp.float32, least / len(shards), high / len(shards))
        level = level * jnp.repeat(jnp.exp(steps), shape[dim] // shards_of).reshape((-1,) + (1,) * (len(shape) - 1 - dim))
    return level


def noise(own_key, extent, scale, reach, cuts=(), held_as=jnp.bfloat16):
    loudness = shard_levels(own_key, extent, cuts, -0.22, 0.18) if cuts else 1.0
    values = jax.random.normal(own_key, extent, jnp.float32) * scale * loudness
    return jnp.minimum(jnp.maximum(values, -reach), reach).astype(held_as)


def setup_inputs(seed: int = 0) -> dict:
    key_of = jax.random.split(jax.random.key(seed), 11)
    return {
        "frames": noise(key_of[0], (FRAMES, D), 1.0, 6.0, ((0, 32),)),
        "ln1_gain": jnp.clip(1.0 + 0.18 * jax.random.normal(key_of[1], (D,), jnp.float32), 0.1, 1.9),
        "w_in": noise(key_of[2], (D, 2, D), D ** -0.5, 0.1875, ((0, 8), (2, 4))),
        "w_dw": noise(key_of[3], (KER, D), KER ** -0.5, 1.0),
        "ln2_gain": jnp.clip(1.0 + 0.18 * jax.random.normal(key_of[4], (D,), jnp.float32), 0.1, 1.9),
        "ln2_bias": noise(key_of[5], (D,), 0.5, 3.0, (), jnp.float32),
        "w_out": noise(key_of[6], (D, D), D ** -0.5, 0.1875, ((0, 4), (1, 8))),
        "block_utt": draw_block_utt(jax.random.fold_in(key_of[10], 71), 0),
        "block_off": draw_block_off(jax.random.fold_in(key_of[10], 71), 0),
        "lengths": draw_lengths(jax.random.fold_in(key_of[10], 71), 0),
    }


epsilon = 1e-05

def frame_keys(block_utt, block_off, lengths, first_row, row_count, margin):
    places = first_row - margin + jnp.arange(row_count + 2 * margin, dtype=jnp.int32)
    total_rows = block_utt.shape[0] * BLK
    inside = (places >= 0) & (places < total_rows)
    blocks = jnp.clip(places // BLK, 0, block_utt.shape[0] - 1)
    utterance = jnp.take(block_utt, blocks)
    position = jnp.take(block_off, blocks) * BLK + places % BLK
    living = inside & (position < jnp.take(lengths, utterance))
    return (jnp.where(living, utterance, -1), living[margin:margin + row_count])

def layer_norm(rows, gain):
    values = rows.astype(jnp.float32)
    average = lax.optimization_barrier(jnp.mean(values, axis=1, keepdims=True))
    centered = values - average
    spread = lax.optimization_barrier(jnp.mean(centered * centered, axis=1, keepdims=True))
    return (centered * lax.rsqrt(spread + epsilon) * gain).astype(jnp.bfloat16)

def gate_units(projected, living):
    half = projected.shape[1] // 2
    values = projected[:, :half] * jax.nn.sigmoid(projected[:, half:])
    return (values * living.astype(jnp.float32)[:, None]).astype(jnp.bfloat16)

def depthwise(widened, keys_wide, taps, row_count):
    margin = (taps.shape[0] - 1) // 2
    center = keys_wide[margin:margin + row_count]
    summed = jnp.zeros((row_count, widened.shape[1]), jnp.float32)
    for tap_index in range(taps.shape[0]):
        shifted = widened[tap_index:tap_index + row_count].astype(jnp.float32)
        same = (keys_wide[tap_index:tap_index + row_count] == center)[:, None]
        summed = summed + jnp.where(same, shifted, 0.0) * taps[tap_index].astype(jnp.float32)
    return summed

def finish(mixed, stat_sum, square_sum, width_total, gain, bias):
    average = stat_sum / width_total
    spread = square_sum / width_total - average * average
    normed = (mixed - average[:, None]) * lax.rsqrt(spread + epsilon)[:, None] * gain + bias
    return (normed * jax.nn.sigmoid(normed)).astype(jnp.bfloat16)

def reference(frames, ln1_gain, w_in, w_dw, ln2_gain, ln2_bias, w_out, block_utt, block_off, lengths):
    margin = (KER - 1) // 2
    keys_wide, living = frame_keys(block_utt, block_off, lengths, 0, FRAMES, margin)
    w_flat = w_in.reshape(D, 2 * D)

    def first_half(pair):
        rows, alive = pair
        normed = layer_norm(rows, ln1_gain)
        projected = jnp.dot(normed, w_flat, preferred_element_type=jnp.float32)
        return gate_units(projected, alive)
    gated = lax.map(first_half, (frames.reshape(N_SEQ, -1, D), living.reshape(N_SEQ, -1))).reshape(FRAMES, D)
    widened = jnp.pad(gated, ((margin, margin), (0, 0)))
    mixed = depthwise(widened, keys_wide, w_dw, FRAMES)

    def second_half(triple):
        rows, alive, mixed_rows = triple
        act = finish(mixed_rows, lax.optimization_barrier(jnp.sum(mixed_rows, axis=1)), lax.optimization_barrier(jnp.sum(mixed_rows * mixed_rows, axis=1)), float(D), ln2_gain, ln2_bias)
        output = jnp.dot(act, w_out, preferred_element_type=jnp.float32)
        return (rows.astype(jnp.float32) + output * alive.astype(jnp.float32)[:, None]).astype(jnp.bfloat16)
    result = lax.map(second_half, (frames.reshape(N_SEQ, -1, D), living.reshape(N_SEQ, -1), mixed.reshape(N_SEQ, -1, D)))
    return result.reshape(FRAMES, D)
```

```python
import functools

import jax
import jax.numpy as jnp
from jax import lax
from jax.experimental import pallas as pl
from jax.experimental.pallas import tpu as pltpu
from jax.sharding import PartitionSpec as P

D = 1024
KER = 31
BLK = 128


epsilon = 1e-05


def extended(block, sides, width):
    for axis, dim in sides:
        count = lax.axis_size(axis)
        forward = [(i, i + 1) for i in range(count - 1)]
        backward = [(target, source) for source, target in forward]
        low = lax.ppermute(
            lax.slice_in_dim(block, block.shape[dim] - width, None, axis=dim), axis, forward
        )
        high = lax.ppermute(lax.slice_in_dim(block, 0, width, axis=dim), axis, backward)
        block = jnp.concatenate([low, block, high], axis=dim)
    return block


def frame_keys(block_utt, block_off, lengths, first_row, row_count, margin):
    places = first_row - margin + jnp.arange(row_count + 2 * margin, dtype=jnp.int32)
    total_rows = block_utt.shape[0] * BLK
    inside = (places >= 0) & (places < total_rows)
    blocks = jnp.clip(places // BLK, 0, block_utt.shape[0] - 1)
    utterance = jnp.take(block_utt, blocks)
    position = jnp.take(block_off, blocks) * BLK + places % BLK
    living = inside & (position < jnp.take(lengths, utterance))
    return (jnp.where(living, utterance, -1), living[margin : margin + row_count])


def layer_norm(rows, gain):
    values = rows.astype(jnp.float32)
    average = jnp.mean(values, axis=1, keepdims=True)
    centered = values - average
    spread = jnp.mean(centered * centered, axis=1, keepdims=True)
    return (centered * lax.rsqrt(spread + epsilon) * gain).astype(jnp.bfloat16)


def gate_units(projected, living):
    half = projected.shape[1] // 2
    values = projected[:, :half] * jax.nn.sigmoid(projected[:, half:])
    return (values * living.astype(jnp.float32)[:, None]).astype(jnp.bfloat16)


def depthwise(widened, keys_wide, taps, row_count):
    margin = (taps.shape[0] - 1) // 2
    center = keys_wide[margin : margin + row_count]
    summed = jnp.zeros((row_count, widened.shape[1]), jnp.float32)
    for tap_index in range(taps.shape[0]):
        shifted = widened[tap_index : tap_index + row_count].astype(jnp.float32)
        same = (keys_wide[tap_index : tap_index + row_count] == center)[:, None]
        summed = summed + jnp.where(same, shifted, 0.0) * taps[tap_index].astype(jnp.float32)
    return summed


def finish(mixed, stat_sum, square_sum, width_total, gain, bias):
    average = stat_sum / width_total
    spread = square_sum / width_total - average * average
    normed = (mixed - average[:, None]) * lax.rsqrt(spread + epsilon)[:, None] * gain + bias
    return (normed * jax.nn.sigmoid(normed)).astype(jnp.bfloat16)


def project_rows(normed, row_count, column_count):

    def add_rows(total, weight_piece, start_row):
        piece_rows = weight_piece.shape[0]
        return jnp.dot(
            normed, weight_piece.reshape(piece_rows, -1), preferred_element_type=jnp.float32
        )

    return (add_rows, jnp.zeros((row_count, column_count), jnp.float32))


def per_device(
    frames, ln1_gain, w_in, w_dw, ln2_gain, ln2_bias, w_out, block_utt, block_off, lengths
):
    row_count = frames.shape[0]
    margin = (KER - 1) // 2
    own_first = lax.axis_index(("seq", "grp")) * row_count
    keys_wide, living = frame_keys(block_utt, block_off, lengths, own_first, row_count, margin)
    normed = layer_norm(frames, ln1_gain)
    w_in_rows, w_out_rows = (
        lax.all_gather(w_in, "grp", axis=2, tiled=True),
        lax.all_gather(w_out, "grp", axis=0, tiled=True),
    )
    add_rows, empty = project_rows(normed, row_count, 2 * D)
    projected = add_rows(empty, lax.all_gather(w_in_rows, "seq", axis=0, tiled=True), jnp.int32(0))
    gated = gate_units(projected, living)
    widened = extended(gated, ((("seq", "grp"), 0),), margin)
    mixed = depthwise(widened, keys_wide, w_dw, row_count)
    act = finish(
        mixed, jnp.sum(mixed, axis=1), jnp.sum(mixed * mixed, axis=1), float(D), ln2_gain, ln2_bias
    )
    output = jnp.dot(
        act,
        lax.all_gather(w_out_rows, "seq", axis=1, tiled=True),
        preferred_element_type=jnp.float32,
    )
    alive = living.astype(jnp.float32)[:, None]
    return (frames.astype(jnp.float32) + output * alive).astype(jnp.bfloat16)


MESH = pl.DeviceIdType.MESH
HALO = 16
LANES = 128


def fused_kernel(
    nz,
    frames_hbm,
    wi_hbm,
    wo_hbm,
    gain1,
    taps,
    gain2,
    bias2,
    utts,
    offs,
    lens,
    out_hbm,
    WI,
    WO,
    FR,
    HB,
    NM,
    GB,
    MX,
    TP,
    ACT,
    OUT,
    ssem,
    rsem,
    hs,
    hr,
    lsem,
    osem,
):
    rows, width = FR.shape
    krows = wi_hbm.shape[0]
    orows, ocols = wo_hbm.shape
    nblk = rows // BLK
    chunks = width // LANES
    per_group = wi_hbm.shape[1] // (2 * LANES)
    seq = lax.axis_index("seq")
    grp = lax.axis_index("grp")
    nseq = lax.axis_size("seq")
    ngrp = lax.axis_size("grp")
    z, y = seq // 2, seq % 2
    x, c = grp // 2, grp % 2
    index = seq * ngrp + grp
    total = nseq * ngrp
    after = (index + 1) % total
    before = (index + total - 1) % total
    px = (seq, (1 - x) * 2 + c)
    py = (z * 2 + 1 - y, grp)
    pp = (seq, x * 2 + 1 - c)
    pn = (after // ngrp, after % ngrp)
    pb = (before // ngrp, before % ngrp)
    up = (jnp.minimum(z + 1, nz - 1) * 2 + y, grp)
    down = (jnp.maximum(z - 1, 0) * 2 + y, grp)
    has_up = z < nz - 1
    has_down = z > 0

    own_in = WI.at[grp, pl.ds(pl.multiple_of(seq * krows, krows), krows), :]
    own_out = WO.at[
        pl.ds(pl.multiple_of(grp * orows, orows), orows),
        pl.ds(pl.multiple_of(seq * ocols, ocols), ocols),
    ]
    load_in = pltpu.make_async_copy(wi_hbm, own_in, lsem.at[0])
    load_out = pltpu.make_async_copy(wo_hbm, own_out, lsem.at[1])
    load_fr = pltpu.make_async_copy(frames_hbm, FR, lsem.at[2])
    load_in.start()
    load_fr.start()
    load_out.start()

    barrier = pltpu.get_barrier_semaphore()
    for peer in (px, py, pp, pn, pb):
        pl.semaphore_signal(barrier, inc=1, device_id=peer, device_id_type=MESH)

    @pl.when(has_up)
    def _():
        pl.semaphore_signal(barrier, inc=1, device_id=up, device_id_type=MESH)

    @pl.when(has_down)
    def _():
        pl.semaphore_signal(barrier, inc=1, device_id=down, device_id_type=MESH)

    load_in.wait()
    pl.semaphore_wait(barrier, 5 + has_up.astype(jnp.int32) + has_down.astype(jnp.int32))

    def slot(w, sx, sy, sz, sc, half=None):
        g = sx * 2 + sc
        s = sz * 2 + sy
        if w == 0:
            count = krows if half is None else krows // 2
            first = s * krows + (0 if half is None else half * count)
            return WI.at[g, pl.ds(pl.multiple_of(first, count), count), :]
        count = orows if half is None else orows // 2
        first = g * orows + (0 if half is None else half * count)
        return WO.at[
            pl.ds(pl.multiple_of(first, count), count),
            pl.ds(pl.multiple_of(s * ocols, ocols), ocols),
        ]

    ZU, ZD = 0, nz - 1
    XD, YD = 2 * nz - 2, 3 * nz - 2
    XH, YH = 4 * nz - 2, 5 * nz - 2
    PO, PY, PX, PXH, PYH = (6 * nz - 2 + i * nz for i in range(5))

    def copy(w, ref, sem, dev):
        return pltpu.make_async_remote_copy(
            src_ref=ref,
            dst_ref=ref,
            send_sem=ssem.at[w, sem],
            recv_sem=rsem.at[w, sem],
            device_id=dev,
            device_id_type=MESH,
        )

    def spread(w, sz):
        ref = slot(w, x, y, sz, c)
        copy(w, ref, XD + sz, px).start()
        copy(w, ref, YD + sz, py).start()
        copy(w, ref, PO + sz, pp).start()

    def first_sends(w):
        ref = slot(w, x, y, z, c)

        @pl.when(has_up)
        def _():
            copy(w, ref, ZU, up).start()

        @pl.when(has_down)
        def _():
            copy(w, ref, ZD, down).start()

        spread(w, z)

    def line(w, d):
        @pl.when(z >= d)
        def _():
            ref = slot(w, x, y, z - d, c)
            copy(w, ref, ZU + d - 1, down).wait_recv()
            if d < nz - 1:

                @pl.when(has_up)
                def _():
                    copy(w, ref, ZU + d, up).start()

            spread(w, z - d)

        @pl.when(z + d < nz)
        def _():
            ref = slot(w, x, y, z + d, c)
            copy(w, ref, ZD + d - 1, up).wait_recv()
            if d < nz - 1:

                @pl.when(has_down)
                def _():
                    copy(w, ref, ZD + d, down).start()

            spread(w, z + d)

    def square_at(w, sz):
        ref = slot(w, x, 1 - y, sz, c)
        copy(w, ref, YD + sz, py).wait_recv()
        copy(w, slot(w, x, 1 - y, sz, c, 0), XH + sz, px).start()
        copy(w, ref, PY + sz, pp).start()
        ref = slot(w, 1 - x, y, sz, c)
        copy(w, ref, XD + sz, px).wait_recv()
        copy(w, slot(w, 1 - x, y, sz, c, 1), YH + sz, py).start()
        copy(w, ref, PX + sz, pp).start()

    def corner_at(w, sz):
        ref = slot(w, 1 - x, 1 - y, sz, c, 0)
        copy(w, ref, XH + sz, px).wait_recv()
        copy(w, ref, PXH + sz, pp).start()
        ref = slot(w, 1 - x, 1 - y, sz, c, 1)
        copy(w, ref, YH + sz, py).wait_recv()
        copy(w, ref, PYH + sz, pp).start()

    def at_distance(step, w, d):
        if d == 0:
            step(w, z)
            return

        @pl.when(z >= d)
        def _():
            step(w, z - d)

        @pl.when(z + d < nz)
        def _():
            step(w, z + d)

    def partner_near(w):
        for sz in range(nz):
            copy(w, slot(w, x, y, sz, 1 - c), PO + sz, pp).wait_recv()
            copy(w, slot(w, x, 1 - y, sz, 1 - c), PY + sz, pp).wait_recv()

    def partner_far(w):
        for sz in range(nz):
            copy(w, slot(w, 1 - x, y, sz, 1 - c), PX + sz, pp).wait_recv()
            copy(w, slot(w, 1 - x, 1 - y, sz, 1 - c, 0), PXH + sz, pp).wait_recv()
            copy(w, slot(w, 1 - x, 1 - y, sz, 1 - c, 1), PYH + sz, pp).wait_recv()

    def halo_copy(src, dst, sem, dev):
        return pltpu.make_async_remote_copy(
            src_ref=src,
            dst_ref=dst,
            send_sem=hs.at[sem],
            recv_sem=hr.at[sem],
            device_id=dev,
            device_id_type=MESH,
        )

    to_next = halo_copy(FR.at[pl.ds(rows - HALO, HALO), :], HB.at[0], 0, pn)
    to_before = halo_copy(FR.at[pl.ds(0, HALO), :], HB.at[1], 1, pb)

    first_sends(0)
    load_fr.wait()
    to_next.start()
    to_before.start()
    load_out.wait()
    first_sends(1)

    for ch in range(chunks):
        TP[ch, 0:KER, :] = taps[:, ch * LANES : (ch + 1) * LANES].astype(jnp.float32)

    def norm_rows(block):
        values = block.astype(jnp.float32)
        average = jnp.mean(values, axis=1, keepdims=True)
        centered = values - average
        spread_ = jnp.mean(centered * centered, axis=1, keepdims=True)
        return (centered * lax.rsqrt(spread_ + epsilon) * gain1[...]).astype(jnp.bfloat16)

    step_rows = 32

    def norm_step(i, carry):
        first = pl.multiple_of(i * step_rows, step_rows)
        NM[pl.ds(pl.multiple_of(first + HALO, HALO), step_rows), :] = norm_rows(
            FR[pl.ds(first, step_rows), :]
        )
        return carry

    lax.fori_loop(0, rows // step_rows, norm_step, 0)

    first_block = index * nblk
    last_block = total * nblk - 1

    def block_info(b):
        u = utts[b]
        return u, lens[u] - offs[b] * BLK

    info = [
        block_info(jnp.clip(first_block + i, 0, last_block)) for i in range(-1, nblk + 1)
    ]
    joined = []
    for i in range(nblk + 1):
        same = info[i][0] == info[i + 1][0]
        if i == 0:
            same = same & (first_block > 0)
        if i == nblk:
            same = same & (first_block + nblk <= last_block)
        joined.append(same.astype(jnp.float32))
    alive_rows = [info[i + 1][1] for i in range(nblk)]

    def tall(count, start):
        return start + lax.broadcasted_iota(jnp.int32, (count, LANES), 0)

    def project(g):
        def chunk_step(h, carry):
            weights = WI[g, :, pl.ds(pl.multiple_of(h * 2 * LANES, 2 * LANES), 2 * LANES)]
            p = jnp.dot(NM[...], weights, preferred_element_type=jnp.float32)
            units = p[:, :LANES] * jax.nn.sigmoid(p[:, LANES:])
            pieces = [
                jnp.where(tall(HALO, BLK - HALO) < info[0][1], units[:HALO], 0.0)
            ]
            for i in range(nblk):
                part = units[HALO + i * BLK : HALO + (i + 1) * BLK]
                pieces.append(jnp.where(tall(BLK, 0) < alive_rows[i], part, 0.0))
            pieces.append(
                jnp.where(tall(HALO, 0) < info[nblk + 1][1], units[HALO + rows :], 0.0)
            )
            pieces = [q.astype(jnp.bfloat16).astype(jnp.float32) for q in pieces]
            stride = BLK + 2 * HALO
            for i in range(nblk):
                base = i * stride
                GB[base : base + HALO, :] = pieces[i][-HALO:] * joined[i]
                GB[base + HALO : base + HALO + BLK, :] = pieces[i + 1]
                GB[base + HALO + BLK : base + stride, :] = pieces[i + 2][:HALO] * joined[i + 1]
            ch = g * per_group + h
            tap = [jnp.broadcast_to(TP[ch, k : k + 1, :], (8, LANES)) for k in range(KER)]
            deep = 4
            per_block = BLK // (8 * deep)

            def conv_step(j, inner):
                i, q = j // per_block, j % per_block
                base = pl.multiple_of(i * stride + q * (8 * deep), 8)
                sums = [None] * deep
                for o in range(8 * (deep - 1) + KER):
                    value = GB[pl.ds(base + (1 + o), 8), :]
                    for t in range(deep):
                        k = o - 8 * t
                        if 0 <= k < KER:
                            term = value * tap[k]
                            sums[t] = term if sums[t] is None else sums[t] + term
                first = pl.multiple_of(j * (8 * deep), 8 * deep)
                for t in range(deep):
                    MX[ch, pl.ds(pl.multiple_of(first + 8 * t, 8), 8), :] = sums[t]
                return inner

            lax.fori_loop(0, nblk * per_block, conv_step, 0)
            return carry

        lax.fori_loop(0, per_group, chunk_step, 0)

    line(0, 1)
    at_distance(square_at, 0, 0)
    line(1, 1)
    for d in range(2, nz):
        line(0, d)
        at_distance(square_at, 0, d - 1)
        line(1, d)
        at_distance(square_at, 1, d - 2)
    to_before.wait_recv()
    to_next.wait_recv()
    NM[0:HALO, :] = norm_rows(HB[0])
    NM[HALO + rows :, :] = norm_rows(HB[1])
    at_distance(square_at, 0, nz - 1)
    at_distance(square_at, 1, nz - 2)
    project(grp)
    at_distance(corner_at, 0, 0)
    at_distance(square_at, 1, nz - 1)
    partner_near(0)
    project(x * 2 + 1 - c)
    for d in range(1, nz):
        at_distance(corner_at, 0, d)
    at_distance(corner_at, 1, 0)
    project((1 - x) * 2 + c)
    partner_far(0)
    for d in range(1, nz - 1):
        at_distance(corner_at, 1, d)
    project((1 - x) * 2 + 1 - c)

    at_distance(corner_at, 1, nz - 1)

    def finish_step(j, carry):
        first = pl.multiple_of(j * step_rows, step_rows)
        parts = [MX[ch, pl.ds(first, step_rows), :] for ch in range(chunks)]
        s1 = parts[0]
        s2 = parts[0] * parts[0]
        for part in parts[1:]:
            s1 = s1 + part
            s2 = s2 + part * part
        average = jnp.sum(s1, axis=1, keepdims=True) / float(width)
        spread_ = jnp.sum(s2, axis=1, keepdims=True) / float(width) - average * average
        scale = lax.rsqrt(spread_ + epsilon)
        for ch in range(chunks):
            cols = slice(ch * LANES, (ch + 1) * LANES)
            v = (parts[ch] - average) * scale * gain2[:, cols] + bias2[:, cols]
            ACT[pl.ds(first, step_rows), cols] = (v * jax.nn.sigmoid(v)).astype(jnp.bfloat16)
        return carry

    lax.fori_loop(0, rows // step_rows, finish_step, 0)

    partner_near(1)
    partner_far(1)

    wide = 2 * LANES

    def out_copy(n):
        cols = pl.ds(pl.multiple_of(n * wide, wide), wide)
        return pltpu.make_async_copy(OUT.at[:, cols], out_hbm.at[:, cols], osem.at[n])

    def out_step(n, carry):
        cols = pl.ds(pl.multiple_of(n * wide, wide), wide)
        o = jnp.dot(ACT[...], WO[:, cols], preferred_element_type=jnp.float32)
        for i in range(nblk):
            band = slice(i * BLK, (i + 1) * BLK)
            lived = (
                lax.broadcasted_iota(jnp.int32, (BLK, wide), 0) < alive_rows[i]
            ).astype(jnp.float32)
            OUT[band, cols] = (
                FR[band, cols].astype(jnp.float32) + o[band] * lived
            ).astype(jnp.bfloat16)
        out_copy(n).start()
        return carry

    lax.fori_loop(0, width // wide, out_step, 0)

    to_next.wait_send()
    to_before.wait_send()
    for w in range(2):
        full = slot(w, x, y, z, c)
        part = slot(w, x, y, z, c, 0)
        for d in range(1, nz):

            @pl.when((z >= d - 1) & has_up)
            def _():
                copy(w, full, ZU + d - 1, up).wait_send()

            @pl.when((z + d - 1 < nz) & has_down)
            def _():
                copy(w, full, ZD + d - 1, down).wait_send()

        for sz in range(nz):
            copy(w, full, XD + sz, px).wait_send()
            copy(w, full, YD + sz, py).wait_send()
            copy(w, part, XH + sz, px).wait_send()
            copy(w, part, YH + sz, py).wait_send()
            copy(w, full, PO + sz, pp).wait_send()
            copy(w, full, PY + sz, pp).wait_send()
            copy(w, full, PX + sz, pp).wait_send()
            copy(w, part, PXH + sz, pp).wait_send()
            copy(w, part, PYH + sz, pp).wait_send()
    for n in range(width // wide):
        out_copy(n).wait()


def fused_device(
    frames, ln1_gain, w_in, w_dw, ln2_gain, ln2_bias, w_out, block_utt, block_off, lengths
):
    rows, width = frames.shape
    nz = lax.axis_size("seq") // 2
    krows, _, cols = w_in.shape
    groups = cols // LANES
    wi = w_in.reshape(krows, 2, groups, LANES).transpose(0, 2, 1, 3).reshape(krows, 2 * cols)
    vmem = pl.BlockSpec(memory_space=pltpu.VMEM)
    smem = pl.BlockSpec(memory_space=pltpu.SMEM)
    anywhere = pl.BlockSpec(memory_space=pl.ANY)
    nsem = 11 * nz - 2
    nblk = rows // BLK
    return pl.pallas_call(
        functools.partial(fused_kernel, nz),
        out_shape=jax.ShapeDtypeStruct((rows, width), jnp.bfloat16),
        in_specs=[anywhere] * 3 + [vmem] * 4 + [smem] * 3,
        out_specs=anywhere,
        scratch_shapes=[
            pltpu.VMEM((width // cols, width, 2 * cols), jnp.bfloat16),
            pltpu.VMEM((width, width), jnp.bfloat16),
            pltpu.VMEM((rows, width), jnp.bfloat16),
            pltpu.VMEM((2, HALO, width), jnp.bfloat16),
            pltpu.VMEM((rows + 2 * HALO, width), jnp.bfloat16),
            pltpu.VMEM((nblk * (BLK + 2 * HALO), LANES), jnp.float32),
            pltpu.VMEM((width // LANES, rows, LANES), jnp.float32),
            pltpu.VMEM((width // LANES, 32, LANES), jnp.float32),
            pltpu.VMEM((rows, width), jnp.bfloat16),
            pltpu.VMEM((rows, width), jnp.bfloat16),
            pltpu.SemaphoreType.DMA((2, nsem)),
            pltpu.SemaphoreType.DMA((2, nsem)),
            pltpu.SemaphoreType.DMA((2,)),
            pltpu.SemaphoreType.DMA((2,)),
            pltpu.SemaphoreType.DMA((3,)),
            pltpu.SemaphoreType.DMA((width // (2 * LANES),)),
        ],
        compiler_params=pltpu.CompilerParams(
            collective_id=0, has_side_effects=True, vmem_limit_bytes=40 << 20
        ),
    )(
        frames,
        wi,
        w_out,
        ln1_gain[None],
        w_dw,
        ln2_gain[None],
        ln2_bias[None],
        block_utt,
        block_off,
        lengths,
    )


def solution(mesh):
    seq, grp = mesh.shape["seq"], mesh.shape["grp"]
    fits = grp == 4 and seq % 2 == 0 and 4 <= seq <= 8 and D % (seq * LANES) == 0

    return jax.shard_map(
        fused_device if fits else per_device,
        mesh=mesh,
        in_specs=(
            P(("seq", "grp"), None),
            P(),
            P("seq", None, "grp"),
            P(),
            P(),
            P(),
            P("grp", "seq"),
            P(),
            P(),
            P(),
        ),
        out_specs=P(("seq", "grp"), None),
        check_vma=False,
    )
```

```python
import functools

import jax
import jax.numpy as jnp
from jax import lax
from jax.experimental import pallas as pl
from jax.experimental.pallas import tpu as pltpu
from jax.sharding import PartitionSpec as P

D = 1024
KER = 31
BLK = 128


epsilon = 1e-05


def extended(block, sides, width):
    for axis, dim in sides:
        count = lax.axis_size(axis)
        forward = [(i, i + 1) for i in range(count - 1)]
        backward = [(target, source) for source, target in forward]
        low = lax.ppermute(
            lax.slice_in_dim(block, block.shape[dim] - width, None, axis=dim), axis, forward
        )
        high = lax.ppermute(lax.slice_in_dim(block, 0, width, axis=dim), axis, backward)
        block = jnp.concatenate([low, block, high], axis=dim)
    return block


def frame_keys(block_utt, block_off, lengths, first_row, row_count, margin):
    places = first_row - margin + jnp.arange(row_count + 2 * margin, dtype=jnp.int32)
    total_rows = block_utt.shape[0] * BLK
    inside = (places >= 0) & (places < total_rows)
    blocks = jnp.clip(places // BLK, 0, block_utt.shape[0] - 1)
    utterance = jnp.take(block_utt, blocks)
    position = jnp.take(block_off, blocks) * BLK + places % BLK
    living = inside & (position < jnp.take(lengths, utterance))
    return (jnp.where(living, utterance, -1), living[margin : margin + row_count])


def layer_norm(rows, gain):
    values = rows.astype(jnp.float32)
    average = jnp.mean(values, axis=1, keepdims=True)
    centered = values - average
    spread = jnp.mean(centered * centered, axis=1, keepdims=True)
    return (centered * lax.rsqrt(spread + epsilon) * gain).astype(jnp.bfloat16)


def gate_units(projected, living):
    half = projected.shape[1] // 2
    values = projected[:, :half] * jax.nn.sigmoid(projected[:, half:])
    return (values * living.astype(jnp.float32)[:, None]).astype(jnp.bfloat16)


def depthwise(widened, keys_wide, taps, row_count):
    margin = (taps.shape[0] - 1) // 2
    center = keys_wide[margin : margin + row_count]
    summed = jnp.zeros((row_count, widened.shape[1]), jnp.float32)
    for tap_index in range(taps.shape[0]):
        shifted = widened[tap_index : tap_index + row_count].astype(jnp.float32)
        same = (keys_wide[tap_index : tap_index + row_count] == center)[:, None]
        summed = summed + jnp.where(same, shifted, 0.0) * taps[tap_index].astype(jnp.float32)
    return summed


def finish(mixed, stat_sum, square_sum, width_total, gain, bias):
    average = stat_sum / width_total
    spread = square_sum / width_total - average * average
    normed = (mixed - average[:, None]) * lax.rsqrt(spread + epsilon)[:, None] * gain + bias
    return (normed * jax.nn.sigmoid(normed)).astype(jnp.bfloat16)


def project_rows(normed, row_count, column_count):

    def add_rows(total, weight_piece, start_row):
        piece_rows = weight_piece.shape[0]
        return jnp.dot(
            normed, weight_piece.reshape(piece_rows, -1), preferred_element_type=jnp.float32
        )

    return (add_rows, jnp.zeros((row_count, column_count), jnp.float32))


def per_device(
    frames, ln1_gain, w_in, w_dw, ln2_gain, ln2_bias, w_out, block_utt, block_off, lengths
):
    row_count = frames.shape[0]
    margin = (KER - 1) // 2
    own_first = lax.axis_index(("seq", "grp")) * row_count
    keys_wide, living = frame_keys(block_utt, block_off, lengths, own_first, row_count, margin)
    normed = layer_norm(frames, ln1_gain)
    w_in_rows, w_out_rows = (
        lax.all_gather(w_in, "grp", axis=2, tiled=True),
        lax.all_gather(w_out, "grp", axis=0, tiled=True),
    )
    add_rows, empty = project_rows(normed, row_count, 2 * D)
    projected = add_rows(empty, lax.all_gather(w_in_rows, "seq", axis=0, tiled=True), jnp.int32(0))
    gated = gate_units(projected, living)
    widened = extended(gated, ((("seq", "grp"), 0),), margin)
    mixed = depthwise(widened, keys_wide, w_dw, row_count)
    act = finish(
        mixed, jnp.sum(mixed, axis=1), jnp.sum(mixed * mixed, axis=1), float(D), ln2_gain, ln2_bias
    )
    output = jnp.dot(
        act,
        lax.all_gather(w_out_rows, "seq", axis=1, tiled=True),
        preferred_element_type=jnp.float32,
    )
    alive = living.astype(jnp.float32)[:, None]
    return (frames.astype(jnp.float32) + output * alive).astype(jnp.bfloat16)


MESH = pl.DeviceIdType.MESH
HALO = 16
LANES = 128


def fused_kernel(
    nz,
    frames_hbm,
    wi_hbm,
    wo_hbm,
    gain1,
    taps,
    gain2,
    bias2,
    utts,
    offs,
    lens,
    out_hbm,
    WI,
    WO,
    FR,
    HB,
    NM,
    GB,
    MX,
    TP,
    ACT,
    OUT,
    ssem,
    rsem,
    hs,
    hr,
    lsem,
    osem,
):
    rows, width = FR.shape
    krows = wi_hbm.shape[0]
    orows, ocols = wo_hbm.shape
    nblk = rows // BLK
    chunks = width // LANES
    per_group = wi_hbm.shape[1] // (2 * LANES)
    seq = lax.axis_index("seq")
    grp = lax.axis_index("grp")
    nseq = lax.axis_size("seq")
    ngrp = lax.axis_size("grp")
    z, y = seq // 2, seq % 2
    x, c = grp // 2, grp % 2
    index = seq * ngrp + grp
    total = nseq * ngrp
    after = (index + 1) % total
    before = (index + total - 1) % total
    px = (seq, (1 - x) * 2 + c)
    py = (z * 2 + 1 - y, grp)
    pp = (seq, x * 2 + 1 - c)
    pn = (after // ngrp, after % ngrp)
    pb = (before // ngrp, before % ngrp)
    up = (jnp.minimum(z + 1, nz - 1) * 2 + y, grp)
    down = (jnp.maximum(z - 1, 0) * 2 + y, grp)
    has_up = z < nz - 1
    has_down = z > 0

    own_in = WI.at[grp, pl.ds(pl.multiple_of(seq * krows, krows), krows), :]
    own_out = WO.at[
        pl.ds(pl.multiple_of(grp * orows, orows), orows),
        pl.ds(pl.multiple_of(seq * ocols, ocols), ocols),
    ]
    load_in = pltpu.make_async_copy(wi_hbm, own_in, lsem.at[0])
    load_out = pltpu.make_async_copy(wo_hbm, own_out, lsem.at[1])
    load_fr = pltpu.make_async_copy(frames_hbm, FR, lsem.at[2])
    load_in.start()
    load_fr.start()
    load_out.start()

    barrier = pltpu.get_barrier_semaphore()
    for peer in (px, py, pp, pn, pb):
        pl.semaphore_signal(barrier, inc=1, device_id=peer, device_id_type=MESH)

    @pl.when(has_up)
    def _():
        pl.semaphore_signal(barrier, inc=1, device_id=up, device_id_type=MESH)

    @pl.when(has_down)
    def _():
        pl.semaphore_signal(barrier, inc=1, device_id=down, device_id_type=MESH)

    load_in.wait()
    pl.semaphore_wait(barrier, 5 + has_up.astype(jnp.int32) + has_down.astype(jnp.int32))

    def slot(w, sx, sy, sz, sc, half=None):
        g = sx * 2 + sc
        s = sz * 2 + sy
        if w == 0:
            count = krows if half is None else krows // 2
            first = s * krows + (0 if half is None else half * count)
            return WI.at[g, pl.ds(pl.multiple_of(first, count), count), :]
        count = orows if half is None else orows // 2
        first = g * orows + (0 if half is None else half * count)
        return WO.at[
            pl.ds(pl.multiple_of(first, count), count),
            pl.ds(pl.multiple_of(s * ocols, ocols), ocols),
        ]

    ZU, ZD = 0, nz - 1
    XD, YD = 2 * nz - 2, 3 * nz - 2
    XH, YH = 4 * nz - 2, 5 * nz - 2
    PO, PY, PX, PXH, PYH = (6 * nz - 2 + i * nz for i in range(5))

    def copy(w, ref, sem, dev):
        return pltpu.make_async_remote_copy(
            src_ref=ref,
            dst_ref=ref,
            send_sem=ssem.at[w, sem],
            recv_sem=rsem.at[w, sem],
            device_id=dev,
            device_id_type=MESH,
        )

    def spread(w, sz):
        ref = slot(w, x, y, sz, c)
        copy(w, ref, XD + sz, px).start()
        copy(w, ref, YD + sz, py).start()
        copy(w, ref, PO + sz, pp).start()

    def first_sends(w):
        ref = slot(w, x, y, z, c)

        @pl.when(has_up)
        def _():
            copy(w, ref, ZU, up).start()

        @pl.when(has_down)
        def _():
            copy(w, ref, ZD, down).start()

        spread(w, z)

    def line(w, d):
        @pl.when(z >= d)
        def _():
            ref = slot(w, x, y, z - d, c)
            copy(w, ref, ZU + d - 1, down).wait_recv()
            if d < nz - 1:

                @pl.when(has_up)
                def _():
                    copy(w, ref, ZU + d, up).start()

            spread(w, z - d)

        @pl.when(z + d < nz)
        def _():
            ref = slot(w, x, y, z + d, c)
            copy(w, ref, ZD + d - 1, up).wait_recv()
            if d < nz - 1:

                @pl.when(has_down)
                def _():
                    copy(w, ref, ZD + d, down).start()

            spread(w, z + d)

    def square_at(w, sz):
        ref = slot(w, x, 1 - y, sz, c)
        copy(w, ref, YD + sz, py).wait_recv()
        copy(w, slot(w, x, 1 - y, sz, c, 0), XH + sz, px).start()
        copy(w, ref, PY + sz, pp).start()
        ref = slot(w, 1 - x, y, sz, c)
        copy(w, ref, XD + sz, px).wait_recv()
        copy(w, slot(w, 1 - x, y, sz, c, 1), YH + sz, py).start()
        copy(w, ref, PX + sz, pp).start()

    def corner_at(w, sz):
        ref = slot(w, 1 - x, 1 - y, sz, c, 0)
        copy(w, ref, XH + sz, px).wait_recv()
        copy(w, ref, PXH + sz, pp).start()
        ref = slot(w, 1 - x, 1 - y, sz, c, 1)
        copy(w, ref, YH + sz, py).wait_recv()
        copy(w, ref, PYH + sz, pp).start()

    def at_distance(step, w, d):
        if d == 0:
            step(w, z)
            return

        @pl.when(z >= d)
        def _():
            step(w, z - d)

        @pl.when(z + d < nz)
        def _():
            step(w, z + d)

    def partner_near(w):
        for sz in range(nz):
            copy(w, slot(w, x, y, sz, 1 - c), PO + sz, pp).wait_recv()
            copy(w, slot(w, x, 1 - y, sz, 1 - c), PY + sz, pp).wait_recv()

    def partner_far(w):
        for sz in range(nz):
            copy(w, slot(w, 1 - x, y, sz, 1 - c), PX + sz, pp).wait_recv()
            copy(w, slot(w, 1 - x, 1 - y, sz, 1 - c, 0), PXH + sz, pp).wait_recv()
            copy(w, slot(w, 1 - x, 1 - y, sz, 1 - c, 1), PYH + sz, pp).wait_recv()

    def halo_copy(src, dst, sem, dev):
        return pltpu.make_async_remote_copy(
            src_ref=src,
            dst_ref=dst,
            send_sem=hs.at[sem],
            recv_sem=hr.at[sem],
            device_id=dev,
            device_id_type=MESH,
        )

    to_next = halo_copy(FR.at[pl.ds(rows - HALO, HALO), :], HB.at[0], 0, pn)
    to_before = halo_copy(FR.at[pl.ds(0, HALO), :], HB.at[1], 1, pb)

    first_sends(0)
    load_fr.wait()
    to_next.start()
    to_before.start()
    load_out.wait()
    first_sends(1)

    for ch in range(chunks):
        TP[ch, 0:KER, :] = taps[:, ch * LANES : (ch + 1) * LANES].astype(jnp.float32)

    def norm_rows(block):
        values = block.astype(jnp.float32)
        average = jnp.mean(values, axis=1, keepdims=True)
        centered = values - average
        spread_ = jnp.mean(centered * centered, axis=1, keepdims=True)
        return (centered * lax.rsqrt(spread_ + epsilon) * gain1[...]).astype(jnp.bfloat16)

    step_rows = 32

    def norm_step(i, carry):
        first = pl.multiple_of(i * step_rows, step_rows)
        NM[pl.ds(pl.multiple_of(first + HALO, HALO), step_rows), :] = norm_rows(
            FR[pl.ds(first, step_rows), :]
        )
        return carry

    lax.fori_loop(0, rows // step_rows, norm_step, 0)

    first_block = index * nblk
    last_block = total * nblk - 1

    def block_info(b):
        u = utts[b]
        return u, lens[u] - offs[b] * BLK

    info = [
        block_info(jnp.clip(first_block + i, 0, last_block)) for i in range(-1, nblk + 1)
    ]
    joined = []
    for i in range(nblk + 1):
        same = info[i][0] == info[i + 1][0]
        if i == 0:
            same = same & (first_block > 0)
        if i == nblk:
            same = same & (first_block + nblk <= last_block)
        joined.append(same.astype(jnp.float32))
    alive_rows = [info[i + 1][1] for i in range(nblk)]

    def tall(count, start):
        return start + lax.broadcasted_iota(jnp.int32, (count, LANES), 0)

    def project(g):
        def chunk_step(h, carry):
            weights = WI[g, :, pl.ds(pl.multiple_of(h * 2 * LANES, 2 * LANES), 2 * LANES)]
            p = jnp.dot(NM[...], weights, preferred_element_type=jnp.float32)
            half = 0.5 * p[:, :LANES]
            units = half + half * jnp.tanh(0.5 * p[:, LANES:])
            pieces = [
                jnp.where(tall(HALO, BLK - HALO) < info[0][1], units[:HALO], 0.0)
            ]
            for i in range(nblk):
                part = units[HALO + i * BLK : HALO + (i + 1) * BLK]
                pieces.append(jnp.where(tall(BLK, 0) < alive_rows[i], part, 0.0))
            pieces.append(
                jnp.where(tall(HALO, 0) < info[nblk + 1][1], units[HALO + rows :], 0.0)
            )
            pieces = [q.astype(jnp.bfloat16).astype(jnp.float32) for q in pieces]
            stride = BLK + 2 * HALO
            for i in range(nblk):
                base = i * stride
                GB[base : base + HALO, :] = pieces[i][-HALO:] * joined[i]
                GB[base + HALO : base + HALO + BLK, :] = pieces[i + 1]
                GB[base + HALO + BLK : base + stride, :] = pieces[i + 2][:HALO] * joined[i + 1]
            ch = g * per_group + h
            tap = [jnp.broadcast_to(TP[ch, k : k + 1, :], (8, LANES)) for k in range(KER)]
            deep = 4
            per_block = BLK // (8 * deep)

            def conv_step(j, inner):
                i, q = j // per_block, j % per_block
                base = pl.multiple_of(i * stride + q * (8 * deep), 8)
                sums = [None] * deep
                for o in range(8 * (deep - 1) + KER):
                    value = GB[pl.ds(base + (1 + o), 8), :]
                    for t in range(deep):
                        k = o - 8 * t
                        if 0 <= k < KER:
                            term = value * tap[k]
                            sums[t] = term if sums[t] is None else sums[t] + term
                first = pl.multiple_of(j * (8 * deep), 8 * deep)
                for t in range(deep):
                    MX[ch, pl.ds(pl.multiple_of(first + 8 * t, 8), 8), :] = sums[t]
                return inner

            lax.fori_loop(0, nblk * per_block, conv_step, 0, unroll=2)
            return carry

        lax.fori_loop(0, per_group, chunk_step, 0)

    line(0, 1)
    at_distance(square_at, 0, 0)
    line(1, 1)
    for d in range(2, nz):
        line(0, d)
        at_distance(square_at, 0, d - 1)
        line(1, d)
        at_distance(square_at, 1, d - 2)
    to_before.wait_recv()
    to_next.wait_recv()
    NM[0:HALO, :] = norm_rows(HB[0])
    NM[HALO + rows :, :] = norm_rows(HB[1])
    at_distance(square_at, 0, nz - 1)
    at_distance(square_at, 1, nz - 2)
    project(grp)
    at_distance(corner_at, 0, 0)
    at_distance(square_at, 1, nz - 1)
    partner_near(0)
    project(x * 2 + 1 - c)
    for d in range(1, nz):
        at_distance(corner_at, 0, d)
    at_distance(corner_at, 1, 0)
    project((1 - x) * 2 + c)
    partner_far(0)
    for d in range(1, nz - 1):
        at_distance(corner_at, 1, d)
    project((1 - x) * 2 + 1 - c)

    at_distance(corner_at, 1, nz - 1)

    def finish_step(j, carry):
        first = pl.multiple_of(j * step_rows, step_rows)
        parts = [MX[ch, pl.ds(first, step_rows), :] for ch in range(chunks)]
        s1 = parts[0]
        s2 = parts[0] * parts[0]
        for part in parts[1:]:
            s1 = s1 + part
            s2 = s2 + part * part
        average = jnp.sum(s1, axis=1, keepdims=True) / float(width)
        spread_ = jnp.sum(s2, axis=1, keepdims=True) / float(width) - average * average
        scale = lax.rsqrt(spread_ + epsilon)
        for ch in range(chunks):
            cols = slice(ch * LANES, (ch + 1) * LANES)
            v = (parts[ch] - average) * scale * gain2[:, cols] + bias2[:, cols]
            v = 0.5 * v
            ACT[pl.ds(first, step_rows), cols] = (v + v * jnp.tanh(v)).astype(jnp.bfloat16)
        return carry

    lax.fori_loop(0, rows // step_rows, finish_step, 0)

    partner_near(1)
    partner_far(1)

    wide = 2 * LANES

    def out_copy(n):
        cols = pl.ds(pl.multiple_of(n * wide, wide), wide)
        return pltpu.make_async_copy(OUT.at[:, cols], out_hbm.at[:, cols], osem.at[n])

    def out_step(n, carry):
        cols = pl.ds(pl.multiple_of(n * wide, wide), wide)
        o = jnp.dot(ACT[...], WO[:, cols], preferred_element_type=jnp.float32)
        for i in range(nblk):
            band = slice(i * BLK, (i + 1) * BLK)
            lived = (
                lax.broadcasted_iota(jnp.int32, (BLK, wide), 0) < alive_rows[i]
            ).astype(jnp.float32)
            out_hbm[band, cols] = (
                FR[band, cols].astype(jnp.float32) + o[band] * lived
            ).astype(jnp.bfloat16)
        return carry

    lax.fori_loop(0, width // wide, out_step, 0)

    to_next.wait_send()
    to_before.wait_send()
    for w in range(2):
        full = slot(w, x, y, z, c)
        part = slot(w, x, y, z, c, 0)
        for d in range(1, nz):

            @pl.when((z >= d - 1) & has_up)
            def _():
                copy(w, full, ZU + d - 1, up).wait_send()

            @pl.when((z + d - 1 < nz) & has_down)
            def _():
                copy(w, full, ZD + d - 1, down).wait_send()

        for sz in range(nz):
            copy(w, full, XD + sz, px).wait_send()
            copy(w, full, YD + sz, py).wait_send()
            copy(w, part, XH + sz, px).wait_send()
            copy(w, part, YH + sz, py).wait_send()
            copy(w, full, PO + sz, pp).wait_send()
            copy(w, full, PY + sz, pp).wait_send()
            copy(w, full, PX + sz, pp).wait_send()
            copy(w, part, PXH + sz, pp).wait_send()
            copy(w, part, PYH + sz, pp).wait_send()


def fused_device(
    frames, ln1_gain, w_in, w_dw, ln2_gain, ln2_bias, w_out, block_utt, block_off, lengths
):
    rows, width = frames.shape
    nz = lax.axis_size("seq") // 2
    krows, _, cols = w_in.shape
    groups = cols // LANES
    wi = w_in.reshape(krows, 2, groups, LANES).transpose(0, 2, 1, 3).reshape(krows, 2 * cols)
    vmem = pl.BlockSpec(memory_space=pltpu.VMEM)
    smem = pl.BlockSpec(memory_space=pltpu.SMEM)
    anywhere = pl.BlockSpec(memory_space=pl.ANY)
    nsem = 11 * nz - 2
    nblk = rows // BLK
    return pl.pallas_call(
        functools.partial(fused_kernel, nz),
        out_shape=jax.ShapeDtypeStruct((rows, width), jnp.bfloat16),
        in_specs=[anywhere] * 3 + [vmem] * 4 + [smem] * 3,
        out_specs=vmem,
        scratch_shapes=[
            pltpu.VMEM((width // cols, width, 2 * cols), jnp.bfloat16),
            pltpu.VMEM((width, width), jnp.bfloat16),
            pltpu.VMEM((rows, width), jnp.bfloat16),
            pltpu.VMEM((2, HALO, width), jnp.bfloat16),
            pltpu.VMEM((rows + 2 * HALO, width), jnp.bfloat16),
            pltpu.VMEM((nblk * (BLK + 2 * HALO), LANES), jnp.float32),
            pltpu.VMEM((width // LANES, rows, LANES), jnp.float32),
            pltpu.VMEM((width // LANES, 32, LANES), jnp.float32),
            pltpu.VMEM((rows, width), jnp.bfloat16),
            pltpu.VMEM((rows, width), jnp.bfloat16),
            pltpu.SemaphoreType.DMA((2, nsem)),
            pltpu.SemaphoreType.DMA((2, nsem)),
            pltpu.SemaphoreType.DMA((2,)),
            pltpu.SemaphoreType.DMA((2,)),
            pltpu.SemaphoreType.DMA((3,)),
            pltpu.SemaphoreType.DMA((width // (2 * LANES),)),
        ],
        compiler_params=pltpu.CompilerParams(
            collective_id=0, has_side_effects=True, vmem_limit_bytes=40 << 20
        ),
    )(
        frames,
        wi,
        w_out,
        ln1_gain[None],
        w_dw,
        ln2_gain[None],
        ln2_bias[None],
        block_utt,
        block_off,
        lengths,
    )


def solution(mesh):
    seq, grp = mesh.shape["seq"], mesh.shape["grp"]
    fits = grp == 4 and seq % 2 == 0 and 4 <= seq <= 8 and D % (seq * LANES) == 0

    return jax.shard_map(
        fused_device if fits else per_device,
        mesh=mesh,
        in_specs=(
            P(("seq", "grp"), None),
            P(),
            P("seq", None, "grp"),
            P(),
            P(),
            P(),
            P("grp", "seq"),
            P(),
            P(),
            P(),
        ),
        out_specs=P(("seq", "grp"), None),
        check_vma=False,
    )
```
